512 devices in a mesh: shot: 16 (over z, core), pair: 2 (over y_lo), space: 16 (over y_hi, x).
Axes of the slice: x: 4, y: 8 (y_hi: 4, y_lo: 2; y = y_hi * 2 + y_lo), z: 8, core: 2. Of those that a mesh axis runs over, the one named last changes fastest.
Arguments:
- states: float32 [16, 2, 2, 256, 128, 128], P('shot', 'pair', None, 'space'), may hold values from -4 to 4
- courant: float32 [256, 128, 128], P('space'), may hold values from 0.05 to 0.2
- records: float32 [16, 12, 256, 128], P('shot', None, 'space'), may hold values from -6 to 6
Outputs:
- imaging: float32 [256, 128, 128], P('space', 'shot', 'pair')
The draws below stay inside these ranges and needn't reach their ends.
All inputs are finite; a program needn't handle non-finite values.
Results may differ from the reference program's by a relative error of at most 0.00002.
Values sent between devices are 32-bit elements; how exact they have to be, the bound alone decides.
A program may use at most 64 MiB of HBM per device.

```python
import math
import jax
import jax.numpy as jnp
from jax import lax

NY = 128
NZ = 128
STEPS = 12
IMAGE_EVERY = 2
NX = 256
SHOTS = 16


def block_scale(stream_key, shape, pieces, smallest, largest):
    level, own = 1.0, jax.random.fold_in(stream_key, 6)
    for position, blocks in pieces:
        draws = jnp.exp(jax.random.uniform(jax.random.fold_in(own, position), (blocks,), jnp.float32, smallest / len(pieces), largest / len(pieces)))
        level = level * jnp.repeat(draws, shape[position] // blocks).reshape([-1 if axis == position else 1 for axis in range(len(shape))])
    return level


def centred(own_key, dims, deviation, limit, shards=(), kind=jnp.bfloat16):
    entries = deviation * jax.random.normal(own_key, dims, jnp.float32)
    if shards:
        entries = entries * block_scale(own_key, dims, shards, -0.22, 0.18)
    return jnp.clip(entries, -limit, limit).astype(kind)


def setup_inputs(seed: int = 0) -> dict:
    keys = jax.random.split(jax.random.key(seed), 4)
    states = centred(keys[0], (SHOTS, 2, 2, NX, NY, NZ), 0.5, 4.0, ((0, 16), (1, 2), (3, 16)), jnp.float32)
    courant = jnp.clip(jnp.exp(math.log(0.2) - 1.3862944 * jax.random.uniform(keys[1], (NX, NY, NZ), jnp.float32) ** block_scale(keys[1], (NX, NY, NZ), ((0, 16),), -0.2, 0.2)), 0.05, 0.2)
    records = centred(keys[2], (SHOTS, STEPS, NX, NY), 1.0, 6.0, ((0, 16), (2, 16)), jnp.float32)
    return {"states": states, "courant": courant, "records": records}


def laplacian(extended, center):
    base = center.ndim - 3

    def along(whole, dim_axis, extent):
        def shifted(start):
            return lax.slice_in_dim(whole, start, start + extent, axis=dim_axis)
        return (-shifted(0) + 16.0 * shifted(1) - 30.0 * shifted(2) + 16.0 * shifted(3) - shifted(4)) / 12.0

    widths_y = [(0, 0)] * base + [(0, 0), (2, 2), (0, 0)]
    widths_z = [(0, 0)] * base + [(0, 0), (0, 0), (2, 2)]
    total = along(extended, base, center.shape[base])
    total = total + along(jnp.pad(center, widths_y), base + 1, center.shape[base + 1])
    total = total + along(jnp.pad(center, widths_z), base + 2, center.shape[base + 2])
    return total


def advance(earlier, current, courant):
    extended = jnp.pad(current, ((2, 2), (0, 0), (0, 0)))
    return 2.0 * current - earlier + courant * laplacian(extended, current)


def reference(states, courant, records):
    total_image = jnp.zeros(courant.shape, jnp.float32)
    weight = IMAGE_EVERY / STEPS
    for shot_index in range(SHOTS):
        source_old = states[shot_index, 0, 0]
        source_now = states[shot_index, 0, 1]
        receiver_old = states[shot_index, 1, 0]
        receiver_now = states[shot_index, 1, 1]
        shot_image = jnp.zeros(courant.shape, jnp.float32)
        for tick_index in range(STEPS):
            advanced = advance(source_old, source_now, courant)
            source_old, source_now = source_now, advanced
            advanced = advance(receiver_old, receiver_now, courant)
            advanced = advanced.at[:, :, 0].add(records[shot_index, tick_index])
            receiver_old, receiver_now = receiver_now, advanced
            if (tick_index + 1) % IMAGE_EVERY == 0:
                shot_image = shot_image + source_now * receiver_now
        total_image = total_image + shot_image * weight
    return total_image
```

```python
import functools

import jax
import jax.numpy as jnp
from jax import lax
from jax.experimental import pallas as pl
from jax.experimental.pallas import tpu as pltpu
from jax.sharding import PartitionSpec as P

STEPS = 12
IMAGE_EVERY = 2
ROUNDS = STEPS // IMAGE_EVERY
PAD = 8
DEEP = 4
ROWS = 32
NEAR, FAR, CENTRE = 16.0 / 12.0, 1.0 / 12.0, 90.0 / 12.0


def kernel(
    shots, states, courant, records, out,
    now, old, speed, inject, halo, recs, rec_halo, column,
    kept, arrived, packed, landed,
    load_sem, state_sem, first_sem, speed_sem, rec_sem, rec_halo_sem,
    halo_send, halo_recv, first_send, speed_send, rec_send, rec_halo_send, state_send,
    snap_send, snap_recv, sum_send, sum_recv,
):
    layers, height = states.shape[1], states.shape[2]
    groups = shots // 2
    last_space = lax.axis_size("space") - 1
    shot, pair, space = (lax.axis_index(name) for name in ("shot", "pair", "space"))
    deep, core = shot // 2, lax.rem(shot, 2)
    home_shot = 2 * deep + pair
    moves = core != pair
    has_left, has_right = space > 0, space < last_space
    rows = pl.ds(PAD, height)
    base = DEEP

    def at(shot_at, pair_at, space_at):
        return {"shot": shot_at, "pair": pair_at, "space": space_at}

    def remote(source, target, send, recv, device):
        return pltpu.make_async_remote_copy(
            src_ref=source, dst_ref=target, send_sem=send, recv_sem=recv,
            device_id=device, device_id_type=pl.DeviceIdType.MESH,
        )

    def place(ref, sem):
        return pltpu.make_async_copy(ref, ref, sem)

    mate = at(2 * deep + (1 - core), pair, space)
    home = at(home_shot, core, space)

    barrier = pltpu.get_barrier_semaphore()

    def greet(device):
        pl.semaphore_signal(barrier, inc=1, device_id=device, device_id_type=pl.DeviceIdType.MESH)

    def greet_sides(shot_at, pair_at):
        @pl.when(has_left)
        def _():
            greet(at(shot_at, pair_at, space - 1))

        @pl.when(has_right)
        def _():
            greet(at(shot_at, pair_at, space + 1))

    greet(mate)
    greet_sides(shot, pair)

    @pl.when(moves)
    def _():
        greet(home)
        greet_sides(home_shot, core)

    me = 2 * deep + pair
    for step in range(1, shots):
        peer = lax.rem(me + step, shots)
        greet(at(2 * (peer // 2) + core, lax.rem(peer, 2), space))

    load_speed = pltpu.make_async_copy(courant, speed.at[pl.ds(2, layers)], load_sem.at[0])
    load_speed.start()
    load_old = pltpu.make_async_copy(states.at[0], old.at[pl.ds(base, layers), rows], load_sem.at[1])
    load_now = pltpu.make_async_copy(states.at[1], now.at[pl.ds(base, layers), rows], load_sem.at[2])
    load_recs = pltpu.make_async_copy(records, recs, load_sem.at[3])

    @pl.when(jnp.logical_not(moves))
    def _():
        load_now.start()
        load_old.start()

    @pl.when(core * pair == 1)
    def _():
        load_recs.start()

    zero = jnp.zeros((PAD, now.shape[2]), jnp.float32)

    @pl.loop(0, now.shape[0])
    def _(layer):
        for field in (now, old):
            field[layer, pl.ds(0, PAD)] = zero
            field[layer, pl.ds(PAD + height, PAD)] = zero

    flat = jnp.zeros((height, now.shape[2]), jnp.float32)

    def clear(ref, first, count):
        @pl.loop(0, count)
        def _(layer):
            ref[first + layer, rows] = flat

    @pl.when(jnp.logical_not(has_left))
    def _():
        clear(now, 0, DEEP)
        clear(old, 0, DEEP)
        speed[0] = flat
        speed[1] = flat
        rec_halo[0] = jnp.zeros(rec_halo.shape[1:], jnp.float32)

    @pl.when(jnp.logical_not(has_right))
    def _():
        clear(now, base + layers, DEEP)
        clear(old, base + layers, DEEP)
        speed[layers + 2] = flat
        speed[layers + 3] = flat
        rec_halo[1] = jnp.zeros(rec_halo.shape[1:], jnp.float32)

    column[...] = jnp.zeros(column.shape, jnp.float32)

    sides = jnp.where(has_left, 1, 0) + jnp.where(has_right, 1, 0)
    pl.semaphore_wait(barrier, shots + sides + jnp.where(moves, 1 + sides, 0))

    move_now = remote(states.at[1], now.at[pl.ds(base, layers), rows], state_send.at[0], state_sem.at[0], home)
    move_old = remote(states.at[0], old.at[pl.ds(base, layers), rows], state_send.at[1], state_sem.at[1], home)

    def edges(side):
        there = space - 1 if side == 0 else space + 1
        first4, first2 = (0, 0) if side == 0 else (layers - DEEP, layers - 2)
        far = at(home_shot, core, there)
        near = at(shot, pair, there)
        old_at = base + layers if side == 0 else base - 2
        speed_at = layers + 2 if side == 0 else 0
        return (
            remote(states.at[1, pl.ds(first4, DEEP)], halo.at[0, 1 - side, :, rows],
                   first_send.at[0, side], halo_recv.at[0, 1 - side], far),
            remote(states.at[0, pl.ds(first2, 2)], old.at[pl.ds(old_at, 2), rows],
                   first_send.at[1, side], first_sem.at[1 - side], far),
            remote(courant.at[pl.ds(first2, 2)], speed.at[pl.ds(speed_at, 2)],
                   speed_send.at[side], speed_sem.at[1 - side], near),
        )

    has = (has_left, has_right)
    for side in range(2):
        @pl.when(has[side])
        def _(side=side):
            for copy in edges(side):
                copy.start()

    @pl.when(moves)
    def _():
        move_now.start()
        move_old.start()

    move_recs = remote(records, recs, rec_send, rec_sem, mate)

    @pl.when(core + pair == 0)
    def _():
        move_recs.start()

    @pl.when(core * (1 - pair) == 1)
    def _():
        place(recs, rec_sem).wait()

    @pl.when(core * pair == 1)
    def _():
        load_recs.wait()

    def rec_edge(side):
        there = space - 1 if side == 0 else space + 1
        first = 0 if side == 0 else layers - 8
        return remote(recs.at[:, pl.ds(first, 8)], rec_halo.at[1 - side],
                      rec_halo_send.at[side], rec_halo_sem.at[1 - side], at(shot, pair, there))

    @pl.when(core == 1)
    def _():
        for side in range(2):
            @pl.when(has[side])
            def _(side=side):
                rec_edge(side).start()

        def lay(target, values):
            column[pl.ds(0, STEPS)] = values
            inject[target] = column[...].T

        @pl.loop(0, layers)
        def _(layer):
            lay(2 + layer, recs[:, layer])

        for side in range(2):
            @pl.when(has[side])
            def _(side=side):
                place(rec_halo.at[side], rec_halo_sem.at[side]).wait()

        lay(0, rec_halo[0, :, 6])
        lay(1, rec_halo[0, :, 7])
        lay(layers + 2, rec_halo[1, :, 0])
        lay(layers + 3, rec_halo[1, :, 1])

    @pl.when(core == 0)
    def _():
        @pl.loop(0, layers + 4)
        def _(layer):
            inject[layer] = flat

    width = now.shape[2]
    strip = min(ROWS, height)
    lane = lax.broadcasted_iota(jnp.int32, (strip, width), 1)

    def tick(cur, prev, first, count, index):
        shift = lax.rem(width - index, width)

        @pl.loop(0, count)
        def _(step):
            layer = first + step
            for part in range(0, height, strip):
                here = pl.ds(PAD + part, strip)
                mid = cur[layer, here]
                near = cur[layer - 1, here] + cur[layer + 1, here]
                far = cur[layer - 2, here] + cur[layer + 2, here]
                near += cur[layer, pl.ds(PAD + part - 1, strip)] + cur[layer, pl.ds(PAD + part + 1, strip)]
                far += cur[layer, pl.ds(PAD + part - 2, strip)] + cur[layer, pl.ds(PAD + part + 2, strip)]
                near += jnp.where(lane >= 1, pltpu.roll(mid, 1, 1), 0.0)
                near += jnp.where(lane < width - 1, pltpu.roll(mid, width - 1, 1), 0.0)
                far += jnp.where(lane >= 2, pltpu.roll(mid, 2, 1), 0.0)
                far += jnp.where(lane < width - 2, pltpu.roll(mid, width - 2, 1), 0.0)
                spread = NEAR * near - FAR * far - CENTRE * mid
                at_speed = layer - (base - 2)
                step_to = 2.0 * mid - prev[layer, here] + speed[at_speed, pl.ds(part, strip)] * spread
                added = pltpu.roll(inject[at_speed, pl.ds(part, strip)], shift, 1)
                prev[layer, here] = step_to + jnp.where(lane == 0, added, 0.0)

    load_speed.wait()

    @pl.when(moves)
    def _():
        place(now.at[pl.ds(base, layers), rows], state_sem.at[0]).wait()
        place(old.at[pl.ds(base, layers), rows], state_sem.at[1]).wait()

    @pl.when(jnp.logical_not(moves))
    def _():
        load_now.wait()
        load_old.wait()

    def halo_out(side, slot):
        there = space - 1 if side == 0 else space + 1
        first = base if side == 0 else base + layers - DEEP
        return remote(now.at[pl.ds(first, DEEP), rows], halo.at[slot, 1 - side, :, rows],
                      halo_send.at[side], halo_recv.at[slot, 1 - side], at(shot, pair, there))

    def snapshot(index, group):
        theirs = pl.ds(PAD + 8 * (2 * group + 1 - core), 8)
        return remote(now.at[pl.ds(base, layers), theirs], arrived.at[index, group],
                      snap_send, snap_recv.at[index], mate)

    def snapshot_sent():
        pltpu.make_async_copy(arrived.at[0], arrived.at[0], snap_send).wait()

    @pl.loop(0, ROUNDS)
    def _(turn):
        slot = lax.rem(turn, 2)
        tick(now, old, base + 2, layers - 4, 2 * turn)

        @pl.when(turn > 0)
        def _():
            snapshot_sent()

        tick(old, now, base + 4, layers - 8, 2 * turn + 1)
        for side in range(2):
            edge = 0 if side == 0 else base + layers

            @pl.when(has[side])
            def _(side=side, edge=edge):
                place(halo.at[slot, side, :, rows], halo_recv.at[slot, side]).wait()

                @pl.loop(0, DEEP)
                def _(layer):
                    now[edge + layer, rows] = halo[slot, side, layer, rows]

                @pl.when(turn == 0)
                def _():
                    at_old = base - 2 if side == 0 else base + layers
                    at_speed = 0 if side == 0 else layers + 2
                    place(old.at[pl.ds(at_old, 2), rows], first_sem.at[side]).wait()
                    place(speed.at[pl.ds(at_speed, 2)], speed_sem.at[side]).wait()

                @pl.when(turn > 0)
                def _():
                    halo_out(side, slot).wait_send()

            tick(now, old, base - 2 if side == 0 else base + layers - 2, 4, 2 * turn)
            tick(old, now, base if side == 0 else base + layers - 4, 4, 2 * turn + 1)

            @pl.when(jnp.logical_and(has[side], turn < ROUNDS - 1))
            def _(side=side):
                halo_out(side, 1 - slot).start()

        @pl.loop(0, groups)
        def _(group):
            snapshot(turn, group).start()

        @pl.loop(0, layers)
        def _(layer):
            for group in range(groups):
                mine = pl.ds(pl.multiple_of(PAD + 8 * (2 * group + core), 8), 8)
                kept[turn, group, layer] = now[base + layer, mine]

    half_layers = layers // 2
    low = lax.broadcasted_iota(jnp.int32, (8, width), 1) < width // 2
    for index in range(ROUNDS):
        place(arrived.at[index], snap_recv.at[index]).wait()
    snapshot_sent()

    def picture(group, layer):
        total = kept[0, group, layer] * arrived[0, group, layer]
        for index in range(1, ROUNDS):
            total += kept[index, group, layer] * arrived[index, group, layer]
        return total * (IMAGE_EVERY / STEPS)

    @pl.loop(0, groups)
    def _(group):
        @pl.loop(0, half_layers)
        def _(layer):
            one, two = picture(group, layer), picture(group, half_layers + layer)
            packed[2 * group, layer] = jnp.where(low, one, pltpu.roll(two, width // 2, 1))
            packed[2 * group + 1, layer] = jnp.where(low, pltpu.roll(one, width // 2, 1), two)

    def share(step):
        peer = lax.rem(me + step, shots)
        return remote(packed.at[peer], landed.at[step - 1], sum_send, sum_recv,
                      at(2 * (peer // 2) + core, lax.rem(peer, 2), space))

    @pl.loop(1, shots)
    def _(step):
        share(step).start()

    place(landed, sum_recv).wait()

    @pl.loop(0, half_layers)
    def _(layer):
        total = packed[me, layer]
        for step in range(shots - 1):
            total += landed[step, layer]
        out[layer] = total[:, : width // 2]
        out[half_layers + layer] = pltpu.roll(total, width // 2, 1)[:, : width // 2]

    place(landed, sum_send).wait()
    for side in range(2):
        @pl.when(has[side])
        def _(side=side):
            for copy in edges(side):
                copy.wait_send()

            @pl.when(core == 1)
            def _():
                rec_edge(side).wait_send()

    @pl.when(moves)
    def _():
        move_now.wait_send()
        move_old.wait_send()

    @pl.when(core + pair == 0)
    def _():
        move_recs.wait_send()


def on_device(states, courant, records):
    shots = lax.axis_size("shot")
    layers, height, width = courant.shape
    groups = shots // 2
    dma = pltpu.SemaphoreType.DMA
    field = pltpu.VMEM((layers + 2 * DEEP, height + 2 * PAD, width), jnp.float32)
    extended = pltpu.VMEM((layers + 4, height, width), jnp.float32)
    any_space = pl.BlockSpec(memory_space=pl.ANY)
    return pl.pallas_call(
        functools.partial(kernel, shots),
        out_shape=jax.ShapeDtypeStruct((layers, height // shots, width // 2), jnp.float32),
        in_specs=[any_space] * 3,
        out_specs=pl.BlockSpec(memory_space=pltpu.VMEM),
        scratch_shapes=[
            field, field, extended, extended,
            pltpu.VMEM((2, 2, DEEP, height + 2 * PAD, width), jnp.float32),
            pltpu.VMEM((STEPS, layers, height), jnp.float32),
            pltpu.VMEM((2, STEPS, 8, height), jnp.float32),
            pltpu.VMEM((width, height), jnp.float32),
            pltpu.VMEM((ROUNDS, groups, layers, 8, width), jnp.float32),
            pltpu.VMEM((ROUNDS, groups, layers, 8, width), jnp.float32),
            pltpu.VMEM((shots, layers // 2, 8, width), jnp.float32),
            pltpu.VMEM((shots - 1, layers // 2, 8, width), jnp.float32),
            dma((4,)), dma((2,)), dma((2,)), dma((2,)), dma, dma((2,)),
            dma((2,)), dma((2, 2)), dma((2, 2)), dma((2,)), dma, dma((2,)), dma((2,)),
            dma, dma((ROUNDS,)), dma, dma,
        ],
        compiler_params=pltpu.CompilerParams(
            collective_id=0, has_side_effects=True, vmem_limit_bytes=60 << 20
        ),
    )(states[0, 0], courant, records[0])


def solution(mesh):
    placed = (
        P("shot", "pair", None, "space", None, None),
        P("space", None, None),
        P("shot", None, "space", None),
    )
    return jax.shard_map(
        on_device, mesh=mesh, in_specs=placed, out_specs=P("space", "shot", "pair"), check_vma=False
    )
```

```python
import functools
import itertools

import jax
import jax.numpy as jnp
from jax import lax
from jax.experimental import pallas as pl
from jax.experimental.pallas import tpu as pltpu
from jax.sharding import PartitionSpec as P

STEPS = 12
IMAGE_EVERY = 2
ROUNDS = STEPS // IMAGE_EVERY
PAD = 8
DEEP = 4
ROW = 4
ROWS = 32
NEAR, FAR, CENTRE = 16.0 / 12.0, 1.0 / 12.0, 90.0 / 12.0


def kernel(
    shots, states, courant, records, out,
    now, old, speed, inject, near_in, far_in, relay_in, recs, rec_halo, column,
    kept, arrived, packed, landed,
    load_sem, state_sem, old_sem, speed_sem, rec_sem, rec_halo_sem,
    near_send, near_recv, far_send, far_recv, relay_send, relay_recv,
    first_send, speed_send, hand_send, rec_send, rec_halo_send, state_send,
    snap_send, snap_recv, inner_send, outer_send, outer_recv, sum_send, sum_recv,
):
    layers, height = states.shape[1], states.shape[2]
    groups = shots // 2
    last_space = lax.axis_size("space") - 1
    shot, pair, space = (lax.axis_index(name) for name in ("shot", "pair", "space"))
    deep, core = shot // 2, lax.rem(shot, 2)
    home_shot = 2 * deep + pair
    moves = core != pair
    has_left, has_right = space > 0, space < last_space
    has = (has_left, has_right)
    column_at = lax.rem(space, ROW)
    at_start, at_end = column_at == 0, column_at == ROW - 1
    above, below = space + ROW <= last_space, space >= ROW
    far_end = (jnp.logical_and(at_start, has_left), jnp.logical_and(at_end, has_right))
    relays = (jnp.logical_and(at_start, above), jnp.logical_and(at_end, below))
    rows = pl.ds(PAD, height)
    base = DEEP

    def at(shot_at, pair_at, space_at):
        return {"shot": shot_at, "pair": pair_at, "space": space_at}

    def remote(source, target, send, recv, device):
        return pltpu.make_async_remote_copy(
            src_ref=source, dst_ref=target, send_sem=send, recv_sem=recv,
            device_id=device, device_id_type=pl.DeviceIdType.MESH,
        )

    def place(ref, sem):
        return pltpu.make_async_copy(ref, ref, sem)

    mate = at(2 * deep + (1 - core), pair, space)
    home = at(home_shot, core, space)

    barrier = pltpu.get_barrier_semaphore()

    def greet(device):
        pl.semaphore_signal(barrier, inc=1, device_id=device, device_id_type=pl.DeviceIdType.MESH)

    def greet_sides(shot_at, pair_at):
        @pl.when(has_left)
        def _():
            greet(at(shot_at, pair_at, space - 1))

        @pl.when(has_right)
        def _():
            greet(at(shot_at, pair_at, space + 1))

    def greet_rows(shot_at, pair_at):
        ends = jnp.logical_or(at_start, at_end)

        @pl.when(jnp.logical_and(ends, above))
        def _():
            greet(at(shot_at, pair_at, space + ROW))

        @pl.when(jnp.logical_and(ends, below))
        def _():
            greet(at(shot_at, pair_at, space - ROW))

    def greet_other_end(shot_at, pair_at):
        @pl.when(at_start)
        def _():
            greet(at(shot_at, pair_at, space + ROW - 1))

        @pl.when(at_end)
        def _():
            greet(at(shot_at, pair_at, space - ROW + 1))

    greet(mate)
    greet_sides(shot, pair)
    greet_rows(shot, pair)
    greet_other_end(shot, pair)

    @pl.when(moves)
    def _():
        greet(home)
        greet_sides(home_shot, core)
        greet_other_end(home_shot, core)

    me = 2 * deep + pair
    for step in range(1, shots):
        peer = lax.rem(me + step, shots)
        greet(at(2 * (peer // 2) + core, lax.rem(peer, 2), space))

    load_speed = pltpu.make_async_copy(courant, speed.at[pl.ds(2, layers)], load_sem.at[0])
    load_speed.start()
    load_old = pltpu.make_async_copy(states.at[0], old.at[pl.ds(base, layers), rows], load_sem.at[1])
    load_now = pltpu.make_async_copy(states.at[1], now.at[pl.ds(base, layers), rows], load_sem.at[2])
    load_recs = pltpu.make_async_copy(records, recs, load_sem.at[3])

    @pl.when(jnp.logical_not(moves))
    def _():
        load_now.start()
        load_old.start()

    @pl.when(core * pair == 1)
    def _():
        load_recs.start()

    zero = jnp.zeros((PAD, now.shape[2]), jnp.float32)

    @pl.loop(0, now.shape[0])
    def _(layer):
        for field in (now, old):
            field[layer, pl.ds(0, PAD)] = zero
            field[layer, pl.ds(PAD + height, PAD)] = zero

    flat = jnp.zeros((height, now.shape[2]), jnp.float32)

    def clear(ref, first, count):
        @pl.loop(0, count)
        def _(layer):
            ref[first + layer, rows] = flat

    @pl.when(jnp.logical_not(has_left))
    def _():
        clear(now, 0, DEEP)
        clear(old, 0, DEEP)
        speed[0] = flat
        speed[1] = flat
        rec_halo[0] = jnp.zeros(rec_halo.shape[1:], jnp.float32)

    @pl.when(jnp.logical_not(has_right))
    def _():
        clear(now, base + layers, DEEP)
        clear(old, base + layers, DEEP)
        speed[layers + 2] = flat
        speed[layers + 3] = flat
        rec_halo[1] = jnp.zeros(rec_halo.shape[1:], jnp.float32)

    column[...] = jnp.zeros(column.shape, jnp.float32)

    sides = jnp.where(has_left, 1, 0) + jnp.where(has_right, 1, 0)
    ends = jnp.where(jnp.logical_or(at_start, at_end), 1, 0)
    rows_near = ends * (jnp.where(above, 1, 0) + jnp.where(below, 1, 0))
    pl.semaphore_wait(
        barrier, shots + sides + rows_near + ends + jnp.where(moves, 1 + sides + ends, 0)
    )

    move_now = remote(states.at[1], now.at[pl.ds(base, layers), rows], state_send.at[0], state_sem.at[0], home)
    move_old = remote(states.at[0], old.at[pl.ds(base, layers), rows], state_send.at[1], state_sem.at[1], home)

    def split(side, source, target, target_sem, relay, send, shot_at, pair_at, act):
        there = space - 1 if side == 0 else space + 1
        over = space + ROW - 1 if side == 0 else space - ROW + 1

        @pl.when(jnp.logical_and(has[side], jnp.logical_not(far_end[side])))
        def _():
            act(remote(source, target, send, target_sem, at(shot_at, pair_at, there)))

        @pl.when(far_end[side])
        def _():
            act(remote(source, relay_in.at[relay], send, relay_recv.at[relay], at(shot_at, pair_at, over)))

    def old_halo(side):
        return old.at[pl.ds(base - 2 if side == 0 else base + layers, 2), rows]

    def first_later(side, act):
        there = space - 1 if side == 0 else space + 1

        @pl.when(has[side])
        def _():
            act(remote(states.at[1, pl.ds(0 if side == 0 else layers - 2, 2)], near_in.at[0, 1 - side],
                       first_send.at[0, side], near_recv.at[0, 1 - side], at(home_shot, core, there)))

        split(side, states.at[1, pl.ds(2 if side == 0 else layers - 4, 2)], far_in.at[0, 1 - side],
              far_recv.at[0, 1 - side], 0, first_send.at[1, side], home_shot, core, act)

    def first_earlier(side, act):
        split(side, states.at[0, pl.ds(0 if side == 0 else layers - 2, 2)], old_halo(1 - side), old_sem.at[1 - side],
              ROUNDS, first_send.at[2, side], home_shot, core, act)

    def speed_halo(side):
        return speed.at[pl.ds(0 if side == 0 else layers + 2, 2)]

    def speed_edge(side):
        there = space - 1 if side == 0 else space + 1
        return remote(courant.at[pl.ds(0 if side == 0 else layers - 2, 2)], speed_halo(1 - side),
                      speed_send.at[side], speed_sem.at[1 - side], at(shot, pair, there))

    def speed_hand(side):
        return remote(speed_halo(side), speed_halo(side), hand_send.at[side], speed_sem.at[side], mate)

    stays = jnp.logical_not(moves)

    for side in range(2):
        first_later(side, lambda copy: copy.start())

    @pl.when(moves)
    def _():
        move_now.start()
        move_old.start()

    for side in range(2):
        first_earlier(side, lambda copy: copy.start())

        @pl.when(jnp.logical_and(has[side], stays))
        def _(side=side):
            speed_edge(side).start()

    move_recs = remote(records, recs, rec_send, rec_sem, mate)

    @pl.when(core + pair == 0)
    def _():
        move_recs.start()

    @pl.when(core * (1 - pair) == 1)
    def _():
        place(recs, rec_sem).wait()

    @pl.when(core * pair == 1)
    def _():
        load_recs.wait()

    def rec_edge(side):
        there = space - 1 if side == 0 else space + 1
        first = 0 if side == 0 else layers - 8
        return remote(recs.at[:, pl.ds(first, 8)], rec_halo.at[1 - side],
                      rec_halo_send.at[side], rec_halo_sem.at[1 - side], at(shot, pair, there))

    @pl.when(core == 1)
    def _():
        for side in range(2):
            @pl.when(has[side])
            def _(side=side):
                rec_edge(side).start()

        def lay(target, values):
            column[pl.ds(0, STEPS)] = values
            inject[target] = column[...].T

        @pl.loop(0, layers)
        def _(layer):
            lay(2 + layer, recs[:, layer])

        for side in range(2):
            @pl.when(has[side])
            def _(side=side):
                place(rec_halo.at[side], rec_halo_sem.at[side]).wait()

        lay(0, rec_halo[0, :, 6])
        lay(1, rec_halo[0, :, 7])
        lay(layers + 2, rec_halo[1, :, 0])
        lay(layers + 3, rec_halo[1, :, 1])

    @pl.when(core == 0)
    def _():
        @pl.loop(0, layers + 4)
        def _(layer):
            inject[layer] = flat

    width = now.shape[2]
    strip = min(ROWS, height)
    lane = lax.broadcasted_iota(jnp.int32, (strip, width), 1)

    def tick(cur, prev, first, count, index):
        shift = lax.rem(width - index, width)

        @pl.loop(0, count // 2)
        def _(step):
            for sub, part in itertools.product(range(2), range(0, height, strip)):
                layer = first + 2 * step + sub
                here = pl.ds(PAD + part, strip)
                mid = cur[layer, here]
                near = cur[layer - 1, here] + cur[layer + 1, here]
                far = cur[layer - 2, here] + cur[layer + 2, here]
                near += cur[layer, pl.ds(PAD + part - 1, strip)] + cur[layer, pl.ds(PAD + part + 1, strip)]
                far += cur[layer, pl.ds(PAD + part - 2, strip)] + cur[layer, pl.ds(PAD + part + 2, strip)]
                near += jnp.where(lane >= 1, pltpu.roll(mid, 1, 1), 0.0)
                near += jnp.where(lane < width - 1, pltpu.roll(mid, width - 1, 1), 0.0)
                far += jnp.where(lane >= 2, pltpu.roll(mid, 2, 1), 0.0)
                far += jnp.where(lane < width - 2, pltpu.roll(mid, width - 2, 1), 0.0)
                spread = NEAR * near - FAR * far - CENTRE * mid
                at_speed = layer - (base - 2)
                step_to = 2.0 * mid - prev[layer, here] + speed[at_speed, pl.ds(part, strip)] * spread
                added = pltpu.roll(inject[at_speed, pl.ds(part, strip)], shift, 1)
                prev[layer, here] = step_to + jnp.where(lane == 0, added, 0.0)

    load_speed.wait()

    @pl.when(moves)
    def _():
        place(now.at[pl.ds(base, layers), rows], state_sem.at[0]).wait()
        place(old.at[pl.ds(base, layers), rows], state_sem.at[1]).wait()

    @pl.when(jnp.logical_not(moves))
    def _():
        load_now.wait()
        load_old.wait()

    def near_out(side, turn):
        there = space - 1 if side == 0 else space + 1
        edge = base if side == 0 else base + layers - 2
        return remote(now.at[pl.ds(edge, 2), rows], near_in.at[turn, 1 - side],
                      near_send.at[side], near_recv.at[turn, 1 - side], at(shot, pair, there))

    def far_out(side, turn, act):
        edge = base + 2 if side == 0 else base + layers - 4
        split(side, now.at[pl.ds(edge, 2), rows], far_in.at[turn, 1 - side], far_recv.at[turn, 1 - side], turn,
              far_send.at[side], shot, pair, act)

    def pass_on(side, turn, act):
        target = at(shot, pair, space + ROW if side == 0 else space - ROW)
        act(turn, remote(relay_in.at[turn], far_in.at[turn, side], relay_send.at[turn], far_recv.at[turn, side], target))

        @pl.when(turn == 0)
        def _():
            act(ROUNDS, remote(relay_in.at[ROUNDS], old_halo(side), relay_send.at[ROUNDS], old_sem.at[side], target))

    def relay_start(index, copy):
        place(relay_in.at[index], relay_recv.at[index]).wait()
        copy.start()

    def take(source, at_layer):
        for layer in range(2):
            now[at_layer + layer, rows] = source[layer]

    quarter = layers // 4
    half = width // 2
    low = lax.broadcasted_iota(jnp.int32, (8, width), 1) < half

    def snapshot(index, send, recv, spans):
        @pl.loop(0, groups)
        def _(group):
            theirs = pl.ds(pl.multiple_of(PAD + 8 * (2 * group + 1 - core), 8), 8)
            for start, count in spans:
                remote(now.at[pl.ds(base + start, count), theirs], arrived.at[index, group, pl.ds(start, count)],
                       send, recv, mate).start()

        for start, count in spans:
            @pl.loop(start, start + count)
            def _(layer):
                for group in range(groups):
                    mine = pl.ds(pl.multiple_of(PAD + 8 * (2 * group + core), 8), 8)
                    kept[index, group, layer] = now[base + layer, mine]

    def snapshot_sent():
        place(arrived.at[0], snap_send).wait()

    def picture(group, layer):
        total = kept[0, group, layer] * arrived[0, group, layer]
        for index in range(1, ROUNDS):
            total += kept[index, group, layer] * arrived[index, group, layer]
        return total * (IMAGE_EVERY / STEPS)

    def share(part, step):
        peer = lax.rem(me + step, shots)
        return remote(packed.at[part, peer], landed.at[part, step - 1], sum_send.at[part], sum_recv.at[part],
                      at(2 * (peer // 2) + core, lax.rem(peer, 2), space))

    def send_image(part):
        one_at, two_at = (quarter, 2 * quarter) if part == 0 else (0, 3 * quarter)

        @pl.loop(0, groups)
        def _(group):
            for q in range(quarter):
                one, two = picture(group, one_at + q), picture(group, two_at + q)
                packed[part, 2 * group, q] = jnp.where(low, one, pltpu.roll(two, half, 1))
                packed[part, 2 * group + 1, q] = jnp.where(low, pltpu.roll(one, half, 1), two)

        @pl.loop(1, shots)
        def _(step):
            share(part, step).start()

    def take_image(part):
        one_at, two_at = (quarter, 2 * quarter) if part == 0 else (0, 3 * quarter)
        place(landed.at[part], sum_recv.at[part]).wait()
        for q in range(quarter):
            total = packed[part, me, q]
            for step in range(shots - 1):
                total += landed[part, step, q]
            out[one_at + q] = total[:, :half]
            out[two_at + q] = pltpu.roll(total, half, 1)[:, :half]

    last = ROUNDS - 1
    inner_rows = arrived.at[last, :, pl.ds(quarter, 2 * quarter)]

    @pl.loop(0, ROUNDS)
    def _(turn):
        even, odd = 2 * turn, 2 * turn + 1
        tick(now, old, base + 2, layers - 4, even)

        @pl.when(turn > 0)
        def _():
            snapshot_sent()

        tick(old, now, base + 4, layers - 8, odd)

        @pl.when(turn == last)
        def _():
            snapshot(last, inner_send, snap_recv.at[last], ((quarter, 2 * quarter),))

        for side in range(2):
            @pl.when(relays[side])
            def _(side=side):
                pass_on(side, turn, relay_start)

        @pl.when(turn == last)
        def _():
            for index in range(last):
                place(arrived.at[index], snap_recv.at[index]).wait()
            place(inner_rows, snap_recv.at[last]).wait()
            send_image(0)

        for side in range(2):
            @pl.when(has[side])
            def _(side=side):
                place(near_in.at[turn, side], near_recv.at[turn, side]).wait()
                take(near_in.at[turn, side], base - 2 if side == 0 else base + layers)

            @pl.when(turn > 0)
            def _(side=side):
                far_out(side, turn, lambda copy: copy.wait_send())

            tick(now, old, base if side == 0 else base + layers - 2, 2, even)
            tick(old, now, base + 2 if side == 0 else base + layers - 4, 2, odd)

            @pl.when(turn < ROUNDS - 1)
            def _(side=side):
                far_out(side, turn + 1, lambda copy: copy.start())

        for side in range(2):
            @pl.when(has[side])
            def _(side=side):
                place(far_in.at[turn, side], far_recv.at[turn, side]).wait()
                take(far_in.at[turn, side], base - 4 if side == 0 else base + layers + 2)

                @pl.when(turn == 0)
                def _():
                    place(old_halo(side), old_sem.at[side]).wait()
                    place(speed_halo(side), speed_sem.at[side]).wait()

                    @pl.when(stays)
                    def _():
                        speed_hand(side).start()

                @pl.when(turn > 0)
                def _():
                    near_out(side, turn).wait_send()

            tick(now, old, base - 2 if side == 0 else base + layers, 2, even)
            tick(old, now, base if side == 0 else base + layers - 2, 2, odd)

            @pl.when(jnp.logical_and(has[side], turn < ROUNDS - 1))
            def _(side=side):
                near_out(side, turn + 1).start()

        @pl.when(turn < last)
        def _():
            snapshot(turn, snap_send, snap_recv.at[turn], ((0, layers),))

        @pl.when(turn == last)
        def _():
            snapshot(last, outer_send, outer_recv, ((0, quarter), (3 * quarter, quarter)))

    place(inner_rows, outer_recv).wait()
    send_image(1)
    take_image(0)
    take_image(1)

    for part in range(2):
        place(landed.at[part], sum_send.at[part]).wait()
    place(inner_rows, inner_send).wait()
    place(inner_rows, outer_send).wait()
    for side in range(2):
        first_later(side, lambda copy: copy.wait_send())
        first_earlier(side, lambda copy: copy.wait_send())

        @pl.when(jnp.logical_and(has[side], stays))
        def _(side=side):
            speed_edge(side).wait_send()
            speed_hand(side).wait_send()

        @pl.when(jnp.logical_and(has[side], core == 1))
        def _(side=side):
            rec_edge(side).wait_send()

        @pl.when(relays[side])
        def _(side=side):
            @pl.loop(0, ROUNDS)
            def _(turn):
                pass_on(side, turn, lambda index, copy: copy.wait_send())

    @pl.when(moves)
    def _():
        move_now.wait_send()
        move_old.wait_send()

    @pl.when(core + pair == 0)
    def _():
        move_recs.wait_send()


def on_device(states, courant, records):
    shots = lax.axis_size("shot")
    layers, height, width = courant.shape
    groups = shots // 2
    dma = pltpu.SemaphoreType.DMA
    field = pltpu.VMEM((layers + 2 * DEEP, height + 2 * PAD, width), jnp.float32)
    extended = pltpu.VMEM((layers + 4, height, width), jnp.float32)
    any_space = pl.BlockSpec(memory_space=pl.ANY)
    return pl.pallas_call(
        functools.partial(kernel, shots),
        out_shape=jax.ShapeDtypeStruct((layers, height // shots, width // 2), jnp.float32),
        in_specs=[any_space] * 3,
        out_specs=pl.BlockSpec(memory_space=pltpu.VMEM),
        scratch_shapes=[
            field, field, extended, extended,
            pltpu.VMEM((ROUNDS, 2, 2, height, width), jnp.float32),
            pltpu.VMEM((ROUNDS, 2, 2, height, width), jnp.float32),
            pltpu.VMEM((ROUNDS + 1, 2, height, width), jnp.float32),
            pltpu.VMEM((STEPS, layers, height), jnp.float32),
            pltpu.VMEM((2, STEPS, 8, height), jnp.float32),
            pltpu.VMEM((width, height), jnp.float32),
            pltpu.VMEM((ROUNDS, groups, layers, 8, width), jnp.float32),
            pltpu.VMEM((ROUNDS, groups, layers, 8, width), jnp.float32),
            pltpu.VMEM((2, shots, layers // 4, 8, width), jnp.float32),
            pltpu.VMEM((2, shots - 1, layers // 4, 8, width), jnp.float32),
            dma((4,)), dma((2,)), dma((2,)), dma((2,)), dma, dma((2,)),
            dma((2,)), dma((ROUNDS, 2)), dma((2,)), dma((ROUNDS, 2)), dma((ROUNDS + 1,)), dma((ROUNDS + 1,)),
            dma((3, 2)), dma((2,)), dma((2,)), dma, dma((2,)), dma((2,)),
            dma, dma((ROUNDS,)), dma, dma, dma, dma((2,)), dma((2,)),
        ],
        compiler_params=pltpu.CompilerParams(
            collective_id=0, has_side_effects=True, vmem_limit_bytes=60 << 20
        ),
    )(states[0, 0], courant, records[0])


def solution(mesh):
    placed = (
        P("shot", "pair", None, "space", None, None),
        P("space", None, None),
        P("shot", None, "space", None),
    )
    return jax.shard_map(
        on_device, mesh=mesh, in_specs=placed, out_specs=P("space", "shot", "pair"), check_vma=False
    )
```

```python
import functools
import itertools

import jax
import jax.numpy as jnp
from jax import lax
from jax.experimental import pallas as pl
from jax.experimental.pallas import tpu as pltpu
from jax.sharding import PartitionSpec as P

STEPS = 12
IMAGE_EVERY = 2
ROUNDS = STEPS // IMAGE_EVERY
PAD = 8
DEEP = 4
ROW = 4
ROWS = 32
NEAR, FAR, CENTRE = 16.0 / 12.0, 1.0 / 12.0, 90.0 / 12.0


def kernel(
    shots, states, courant, records, out,
    now, old, speed, inject, near_in, far_in, relay_in, recs, rec_halo, column,
    kept, arrived, packed, landed,
    load_sem, state_sem, old_sem, speed_sem, rec_sem, rec_halo_sem,
    near_send, near_recv, far_send, far_recv, relay_send, relay_recv,
    first_send, speed_send, hand_send, rec_send, rec_halo_send, state_send,
    snap_send, snap_recv, inner_send, outer_send, outer_recv, sum_send, sum_recv, clear_road,
):
    layers, height = states.shape[1], states.shape[2]
    groups = shots // 2
    last_space = lax.axis_size("space") - 1
    shot, pair, space = (lax.axis_index(name) for name in ("shot", "pair", "space"))
    deep, core = shot // 2, lax.rem(shot, 2)
    home_shot = 2 * deep + pair
    moves = core != pair
    has_left, has_right = space > 0, space < last_space
    has = (has_left, has_right)
    column_at = lax.rem(space, ROW)
    at_start, at_end = column_at == 0, column_at == ROW - 1
    above, below = space + ROW <= last_space, space >= ROW
    far_end = (jnp.logical_and(at_start, has_left), jnp.logical_and(at_end, has_right))
    relays = (jnp.logical_and(at_start, above), jnp.logical_and(at_end, below))
    rows = pl.ds(PAD, height)
    base = DEEP

    def at(shot_at, pair_at, space_at):
        return {"shot": shot_at, "pair": pair_at, "space": space_at}

    def remote(source, target, send, recv, device):
        return pltpu.make_async_remote_copy(
            src_ref=source, dst_ref=target, send_sem=send, recv_sem=recv,
            device_id=device, device_id_type=pl.DeviceIdType.MESH,
        )

    def place(ref, sem):
        return pltpu.make_async_copy(ref, ref, sem)

    def begin(copy):
        copy.start()

    def sent(copy):
        copy.wait_send()

    mate = at(2 * deep + (1 - core), pair, space)
    home = at(home_shot, core, space)

    barrier = pltpu.get_barrier_semaphore()

    def greet(device):
        pl.semaphore_signal(barrier, inc=1, device_id=device, device_id_type=pl.DeviceIdType.MESH)

    def greet_sides(shot_at, pair_at):
        @pl.when(has_left)
        def _():
            greet(at(shot_at, pair_at, space - 1))

        @pl.when(has_right)
        def _():
            greet(at(shot_at, pair_at, space + 1))

    def greet_rows(shot_at, pair_at):
        ends = jnp.logical_or(at_start, at_end)

        @pl.when(jnp.logical_and(ends, above))
        def _():
            greet(at(shot_at, pair_at, space + ROW))

        @pl.when(jnp.logical_and(ends, below))
        def _():
            greet(at(shot_at, pair_at, space - ROW))

    def greet_other_end(shot_at, pair_at):
        @pl.when(at_start)
        def _():
            greet(at(shot_at, pair_at, space + ROW - 1))

        @pl.when(at_end)
        def _():
            greet(at(shot_at, pair_at, space - ROW + 1))

    greet(mate)
    greet_sides(shot, pair)
    greet_rows(shot, pair)
    greet_other_end(shot, pair)

    @pl.when(moves)
    def _():
        greet(home)
        greet_sides(home_shot, core)
        greet_other_end(home_shot, core)

    me = 2 * deep + pair
    for step in range(1, shots):
        peer = lax.rem(me + step, shots)
        greet(at(2 * (peer // 2) + core, lax.rem(peer, 2), space))

    load_speed = pltpu.make_async_copy(courant, speed.at[pl.ds(2, layers)], load_sem.at[0])
    load_speed.start()
    load_old = pltpu.make_async_copy(states.at[0], old.at[pl.ds(base, layers), rows], load_sem.at[1])
    load_now = pltpu.make_async_copy(states.at[1], now.at[pl.ds(base, layers), rows], load_sem.at[2])
    load_recs = pltpu.make_async_copy(records, recs, load_sem.at[3])

    @pl.when(jnp.logical_not(moves))
    def _():
        load_now.start()
        load_old.start()

    @pl.when(core * pair == 1)
    def _():
        load_recs.start()

    zero = jnp.zeros((PAD, now.shape[2]), jnp.float32)

    @pl.loop(0, now.shape[0])
    def _(layer):
        for field in (now, old):
            field[layer, pl.ds(0, PAD)] = zero
            field[layer, pl.ds(PAD + height, PAD)] = zero

    flat = jnp.zeros((height, now.shape[2]), jnp.float32)

    def clear(ref, first, count):
        @pl.loop(0, count)
        def _(layer):
            ref[first + layer, rows] = flat

    @pl.when(jnp.logical_not(has_left))
    def _():
        clear(now, 0, DEEP)
        clear(old, 0, DEEP)
        speed[0] = flat
        speed[1] = flat
        rec_halo[0] = jnp.zeros(rec_halo.shape[1:], jnp.float32)

    @pl.when(jnp.logical_not(has_right))
    def _():
        clear(now, base + layers, DEEP)
        clear(old, base + layers, DEEP)
        speed[layers + 2] = flat
        speed[layers + 3] = flat
        rec_halo[1] = jnp.zeros(rec_halo.shape[1:], jnp.float32)

    column[...] = jnp.zeros(column.shape, jnp.float32)

    sides = jnp.where(has_left, 1, 0) + jnp.where(has_right, 1, 0)
    ends = jnp.where(jnp.logical_or(at_start, at_end), 1, 0)
    rows_near = ends * (jnp.where(above, 1, 0) + jnp.where(below, 1, 0))
    pl.semaphore_wait(
        barrier, shots + sides + rows_near + ends + jnp.where(moves, 1 + sides + ends, 0)
    )

    move_now = remote(states.at[1], now.at[pl.ds(base, layers), rows], state_send.at[0], state_sem.at[0], home)
    move_old = remote(states.at[0], old.at[pl.ds(base, layers), rows], state_send.at[1], state_sem.at[1], home)

    def by_layer(act, source, target, send, recv, device):
        if act is begin:
            for layer in range(2):
                one = pl.ds(layer, 1)
                remote(source.at[one], target.at[one], send, recv.at[layer], device).start()
        else:
            act(remote(source, target, send, recv.at[0], device))

    def split(side, source, target, target_sem, relay, send, shot_at, pair_at, act):
        there = space - 1 if side == 0 else space + 1
        over = space + ROW - 1 if side == 0 else space - ROW + 1

        @pl.when(jnp.logical_and(has[side], jnp.logical_not(far_end[side])))
        def _():
            act(remote(source, target, send, target_sem, at(shot_at, pair_at, there)))

        @pl.when(far_end[side])
        def _():
            by_layer(act, source, relay_in.at[relay], send, relay_recv.at[relay], at(shot_at, pair_at, over))

    def old_halo(side):
        return old.at[pl.ds(base - 2 if side == 0 else base + layers, 2), rows]

    def first_later(side, act):
        there = space - 1 if side == 0 else space + 1

        @pl.when(has[side])
        def _():
            act(remote(states.at[1, pl.ds(0 if side == 0 else layers - 2, 2)], near_in.at[0, 1 - side],
                       first_send.at[0, side], near_recv.at[0, 1 - side], at(home_shot, core, there)))

        split(side, states.at[1, pl.ds(2 if side == 0 else layers - 4, 2)], far_in.at[0, 1 - side],
              far_recv.at[0, 1 - side], 0, first_send.at[1, side], home_shot, core, act)

    def first_earlier(side, act):
        split(side, states.at[0, pl.ds(0 if side == 0 else layers - 2, 2)], old_halo(1 - side), old_sem.at[1 - side],
              ROUNDS, first_send.at[2, side], home_shot, core, act)

    def speed_halo(side):
        return speed.at[pl.ds(0 if side == 0 else layers + 2, 2)]

    def speed_edge(side):
        there = space - 1 if side == 0 else space + 1
        return remote(courant.at[pl.ds(0 if side == 0 else layers - 2, 2)], speed_halo(1 - side),
                      speed_send.at[side], speed_sem.at[1 - side], at(shot, pair, there))

    def speed_hand(side):
        return remote(speed_halo(side), speed_halo(side), hand_send.at[side], speed_sem.at[side], mate)

    stays = jnp.logical_not(moves)

    for side in range(2):
        first_later(side, begin)

    @pl.when(moves)
    def _():
        move_now.start()
        move_old.start()

    for side in range(2):
        first_earlier(side, begin)

        @pl.when(jnp.logical_and(has[side], stays))
        def _(side=side):
            speed_edge(side).start()

    move_recs = remote(records, recs, rec_send, rec_sem, mate)

    @pl.when(core + pair == 0)
    def _():
        move_recs.start()

    @pl.when(core * (1 - pair) == 1)
    def _():
        place(recs, rec_sem).wait()

    @pl.when(core * pair == 1)
    def _():
        load_recs.wait()

    def rec_edge(side):
        there = space - 1 if side == 0 else space + 1
        first = 0 if side == 0 else layers - 8
        return remote(recs.at[:, pl.ds(first, 8)], rec_halo.at[1 - side],
                      rec_halo_send.at[side], rec_halo_sem.at[1 - side], at(shot, pair, there))

    @pl.when(core == 1)
    def _():
        for side in range(2):
            @pl.when(has[side])
            def _(side=side):
                rec_edge(side).start()

        def lay(target, values):
            column[pl.ds(0, STEPS)] = values
            inject[target] = column[...].T

        @pl.loop(0, layers)
        def _(layer):
            lay(2 + layer, recs[:, layer])

        for side in range(2):
            @pl.when(has[side])
            def _(side=side):
                place(rec_halo.at[side], rec_halo_sem.at[side]).wait()

        lay(0, rec_halo[0, :, 6])
        lay(1, rec_halo[0, :, 7])
        lay(layers + 2, rec_halo[1, :, 0])
        lay(layers + 3, rec_halo[1, :, 1])

    @pl.when(core == 0)
    def _():
        @pl.loop(0, layers + 4)
        def _(layer):
            inject[layer] = flat

    width = now.shape[2]
    strip = min(ROWS, height)
    lane = lax.broadcasted_iota(jnp.int32, (strip, width), 1)

    def tick(cur, prev, first, count, index):
        shift = lax.rem(width - index, width)

        @pl.loop(0, count // 2)
        def _(step):
            for sub, part in itertools.product(range(2), range(0, height, strip)):
                layer = first + 2 * step + sub
                here = pl.ds(PAD + part, strip)
                mid = cur[layer, here]
                near = cur[layer - 1, here] + cur[layer + 1, here]
                far = cur[layer - 2, here] + cur[layer + 2, here]
                near += cur[layer, pl.ds(PAD + part - 1, strip)] + cur[layer, pl.ds(PAD + part + 1, strip)]
                far += cur[layer, pl.ds(PAD + part - 2, strip)] + cur[layer, pl.ds(PAD + part + 2, strip)]
                near += jnp.where(lane >= 1, pltpu.roll(mid, 1, 1), 0.0)
                near += jnp.where(lane < width - 1, pltpu.roll(mid, width - 1, 1), 0.0)
                far += jnp.where(lane >= 2, pltpu.roll(mid, 2, 1), 0.0)
                far += jnp.where(lane < width - 2, pltpu.roll(mid, width - 2, 1), 0.0)
                spread = NEAR * near - FAR * far - CENTRE * mid
                at_speed = layer - (base - 2)
                step_to = 2.0 * mid - prev[layer, here] + speed[at_speed, pl.ds(part, strip)] * spread
                added = pltpu.roll(inject[at_speed, pl.ds(part, strip)], shift, 1)
                prev[layer, here] = step_to + jnp.where(lane == 0, added, 0.0)

    def near_out(side, turn):
        there = space - 1 if side == 0 else space + 1
        edge = base if side == 0 else base + layers - 2
        return remote(now.at[pl.ds(edge, 2), rows], near_in.at[turn, 1 - side],
                      near_send.at[side], near_recv.at[turn, 1 - side], at(shot, pair, there))

    def far_out(side, turn, act):
        edge = base + 2 if side == 0 else base + layers - 4
        split(side, now.at[pl.ds(edge, 2), rows], far_in.at[turn, 1 - side], far_recv.at[turn, 1 - side], turn,
              far_send.at[side], shot, pair, act)

    def relay_target(side):
        return at(shot, pair, space + ROW if side == 0 else space - ROW)

    def forward(index, target, recv, side):
        for layer in range(2):
            one = pl.ds(layer, 1)
            place(relay_in.at[index, one], relay_recv.at[index, layer]).wait()
            remote(relay_in.at[index, one], target.at[one], relay_send.at[index], recv, relay_target(side)).start()

    def pass_on(side, turn):
        forward(turn, far_in.at[turn, side], far_recv.at[turn, side], side)

    for side in range(2):
        @pl.when(relays[side])
        def _(side=side):
            pass_on(side, 0)
            forward(ROUNDS, old_halo(side), old_sem.at[side], side)

    load_speed.wait()

    @pl.when(moves)
    def _():
        place(now.at[pl.ds(base, layers), rows], state_sem.at[0]).wait()
        place(old.at[pl.ds(base, layers), rows], state_sem.at[1]).wait()
        pl.semaphore_signal(clear_road, inc=1, device_id=mate, device_id_type=pl.DeviceIdType.MESH)

    @pl.when(jnp.logical_not(moves))
    def _():
        load_now.wait()
        load_old.wait()

    def take(source, at_layer):
        for layer in range(2):
            now[at_layer + layer, rows] = source[layer]

    half = width // 2
    low = lax.broadcasted_iota(jnp.int32, (8, width), 1) < half

    def snapshot(index, send, recv, spans):
        @pl.loop(0, groups)
        def _(group):
            theirs = pl.ds(pl.multiple_of(PAD + 8 * (2 * group + 1 - core), 8), 8)
            for start, count in spans:
                remote(now.at[pl.ds(base + start, count), theirs], arrived.at[index, group, pl.ds(start, count)],
                       send, recv, mate).start()

        for start, count in spans:
            @pl.loop(start, start + count)
            def _(layer):
                for group in range(groups):
                    mine = pl.ds(pl.multiple_of(PAD + 8 * (2 * group + core), 8), 8)
                    kept[index, group, layer] = now[base + layer, mine]

    def snapshot_sent():
        place(arrived.at[0], snap_send).wait()

    def picture(group, layer):
        total = kept[0, group, layer] * arrived[0, group, layer]
        for index in range(1, ROUNDS):
            total += kept[index, group, layer] * arrived[index, group, layer]
        return total * (IMAGE_EVERY / STEPS)

    def share(part, step):
        peer = lax.rem(me + step, shots)
        return remote(packed.at[part, peer], landed.at[part, step - 1], sum_send.at[part], sum_recv.at[part],
                      at(2 * (peer // 2) + core, lax.rem(peer, 2), space))

    def send_image(part):
        one_at, two_at = pairs_at[part]

        @pl.loop(0, groups)
        def _(group):
            for q in range(2):
                one, two = picture(group, one_at + q), picture(group, two_at + q)
                packed[part, 2 * group, q] = jnp.where(low, one, pltpu.roll(two, half, 1))
                packed[part, 2 * group + 1, q] = jnp.where(low, pltpu.roll(one, half, 1), two)

        @pl.loop(1, shots)
        def _(step):
            share(part, step).start()

    def take_image(part):
        one_at, two_at = pairs_at[part]
        place(landed.at[part], sum_recv.at[part]).wait()
        for q in range(2):
            total = packed[part, me, q]
            for step in range(shots - 1):
                total += landed[part, step, q]
            out[one_at + q] = total[:, :half]
            out[two_at + q] = pltpu.roll(total, half, 1)[:, :half]

    last = ROUNDS - 1
    pairs_at = ((4, layers - 8), (6, layers - 6), (2, layers - 4), (0, layers - 2))
    inner_rows = arrived.at[last, :, pl.ds(4, layers - 8)]
    outer_rows = arrived.at[last, :, pl.ds(0, 4)]

    @pl.loop(0, ROUNDS)
    def _(turn):
        even, odd = 2 * turn, 2 * turn + 1
        tick(now, old, base + 2, layers - 4, even)

        @pl.when(turn > 0)
        def _():
            snapshot_sent()

        tick(old, now, base + 4, layers - 8, odd)

        @pl.when(turn == last)
        def _():
            snapshot(last, inner_send, snap_recv.at[last], ((4, layers - 8),))

        @pl.when(turn == last)
        def _():
            for index in range(last):
                place(arrived.at[index], snap_recv.at[index]).wait()
            place(inner_rows, snap_recv.at[last]).wait()
            send_image(0)
            send_image(1)

        @pl.when(jnp.logical_and(turn == 0, stays))
        def _():
            pl.semaphore_wait(clear_road, 1)

        for side in range(2):
            @pl.when(has[side])
            def _(side=side):
                place(near_in.at[turn, side], near_recv.at[turn, side]).wait()
                take(near_in.at[turn, side], base - 2 if side == 0 else base + layers)

            @pl.when(turn > 0)
            def _(side=side):
                far_out(side, turn, sent)

            tick(now, old, base if side == 0 else base + layers - 2, 2, even)
            tick(old, now, base + 2 if side == 0 else base + layers - 4, 2, odd)

            @pl.when(turn < ROUNDS - 1)
            def _(side=side):
                far_out(side, turn + 1, begin)

        @pl.when(turn == last)
        def _():
            snapshot(last, outer_send.at[0], outer_recv.at[0], ((2, 2), (layers - 4, 2)))
            place(outer_rows, outer_recv.at[0]).wait()
            send_image(2)

        for side in range(2):
            @pl.when(has[side])
            def _(side=side):
                place(far_in.at[turn, side], far_recv.at[turn, side]).wait()
                take(far_in.at[turn, side], base - 4 if side == 0 else base + layers + 2)

                @pl.when(turn == 0)
                def _():
                    place(old_halo(side), old_sem.at[side]).wait()
                    place(speed_halo(side), speed_sem.at[side]).wait()

                    @pl.when(stays)
                    def _():
                        speed_hand(side).start()

                @pl.when(turn > 0)
                def _():
                    near_out(side, turn).wait_send()

            tick(now, old, base - 2 if side == 0 else base + layers, 2, even)
            tick(old, now, base if side == 0 else base + layers - 2, 2, odd)

            @pl.when(jnp.logical_and(has[side], turn < ROUNDS - 1))
            def _(side=side):
                near_out(side, turn + 1).start()

        for side in range(2):
            @pl.when(jnp.logical_and(relays[side], turn < last))
            def _(side=side):
                pass_on(side, turn + 1)

        @pl.when(turn < last)
        def _():
            snapshot(turn, snap_send, snap_recv.at[turn], ((0, layers),))

        @pl.when(turn == last)
        def _():
            snapshot(last, outer_send.at[1], outer_recv.at[1], ((0, 2), (layers - 2, 2)))

    place(outer_rows, outer_recv.at[1]).wait()
    send_image(3)
    for part in range(4):
        take_image(part)

    for part in range(4):
        place(landed.at[part], sum_send.at[part]).wait()
    place(inner_rows, inner_send).wait()
    for index in range(2):
        place(outer_rows, outer_send.at[index]).wait()
    for side in range(2):
        first_later(side, sent)
        first_earlier(side, sent)

        @pl.when(jnp.logical_and(has[side], stays))
        def _(side=side):
            speed_edge(side).wait_send()
            speed_hand(side).wait_send()

        @pl.when(jnp.logical_and(has[side], core == 1))
        def _(side=side):
            rec_edge(side).wait_send()

        @pl.when(relays[side])
        def _(side=side):
            @pl.loop(0, ROUNDS + 1)
            def _(index):
                place(relay_in.at[index], relay_send.at[index]).wait()

    @pl.when(moves)
    def _():
        move_now.wait_send()
        move_old.wait_send()

    @pl.when(core + pair == 0)
    def _():
        move_recs.wait_send()


def on_device(states, courant, records):
    shots = lax.axis_size("shot")
    layers, height, width = courant.shape
    groups = shots // 2
    dma = pltpu.SemaphoreType.DMA
    field = pltpu.VMEM((layers + 2 * DEEP, height + 2 * PAD, width), jnp.float32)
    extended = pltpu.VMEM((layers + 4, height, width), jnp.float32)
    any_space = pl.BlockSpec(memory_space=pl.ANY)
    return pl.pallas_call(
        functools.partial(kernel, shots),
        out_shape=jax.ShapeDtypeStruct((layers, height // shots, width // 2), jnp.float32),
        in_specs=[any_space] * 3,
        out_specs=pl.BlockSpec(memory_space=pltpu.VMEM),
        scratch_shapes=[
            field, field, extended, extended,
            pltpu.VMEM((ROUNDS, 2, 2, height, width), jnp.float32),
            pltpu.VMEM((ROUNDS, 2, 2, height, width), jnp.float32),
            pltpu.VMEM((ROUNDS + 1, 2, height, width), jnp.float32),
            pltpu.VMEM((STEPS, layers, height), jnp.float32),
            pltpu.VMEM((2, STEPS, 8, height), jnp.float32),
            pltpu.VMEM((width, height), jnp.float32),
            pltpu.VMEM((ROUNDS, groups, layers, 8, width), jnp.float32),
            pltpu.VMEM((ROUNDS, groups, layers, 8, width), jnp.float32),
            pltpu.VMEM((4, shots, 2, 8, width), jnp.float32),
            pltpu.VMEM((4, shots - 1, 2, 8, width), jnp.float32),
            dma((4,)), dma((2,)), dma((2,)), dma((2,)), dma, dma((2,)),
            dma((2,)), dma((ROUNDS, 2)), dma((2,)), dma((ROUNDS, 2)), dma((ROUNDS + 1,)), dma((ROUNDS + 1, 2)),
            dma((3, 2)), dma((2,)), dma((2,)), dma, dma((2,)), dma((2,)),
            dma, dma((ROUNDS,)), dma, dma((2,)), dma((2,)), dma((4,)), dma((4,)),
            pltpu.SemaphoreType.REGULAR,
        ],
        compiler_params=pltpu.CompilerParams(
            collective_id=0, has_side_effects=True, vmem_limit_bytes=60 << 20
        ),
    )(states[0, 0], courant, records[0])


def solution(mesh):
    placed = (
        P("shot", "pair", None, "space", None, None),
        P("space", None, None),
        P("shot", None, "space", None),
    )
    return jax.shard_map(
        on_device, mesh=mesh, in_specs=placed, out_specs=P("space", "shot", "pair"), check_vma=False
    )
```
